32 devices in a mesh: groups: 2 (over y), section: 2 (over core), rank: 8 (over z, x).
Axes of the slice: x: 2, y: 2, z: 4, core: 2. Of those that a mesh axis runs over, the one named last changes fastest.
Arguments:
- rows_in: float32 [2, 16, 8192], P('section', ('groups', 'rank')), parts along dimension 1, may hold values from -54 to 54
- query: bfloat16 [2, 16, 8192], P('section', ('groups', 'rank')), parts along dimension 1, may hold values from -6 to 6
- key_cache: bfloat16 [2, 16, 256, 1024], P('section', ('groups', 'rank')), parts along dimension 1, may hold values from -6 to 6
- value_cache: bfloat16 [2, 16, 256, 1024], P('section', ('groups', 'rank')), parts along dimension 1, may hold values from -6 to 6
- key_new: bfloat16 [2, 16, 1024], P('section', ('groups', 'rank')), parts along dimension 1, may hold values from -6 to 6
- value_new: bfloat16 [2, 16, 1024], P('section', ('groups', 'rank')), parts along dimension 1, may hold values from -6 to 6
- lengths: int32 [2, 16], P('section', ('groups', 'rank')), parts along dimension 1, may hold values from 1 to 256, as said below
- norm_gain: float32 [2, 8192], P('section'), may hold values from 0.25 to 1.75
- w_up: bfloat16 [2, 8192, 14336], P('section', None, 'rank'), may hold values from -0.0625 to 0.0625
- w_down: bfloat16 [2, 14336, 8192], P('section', 'rank'), may hold values from -0.046875 to 0.046875
Outputs:
- next_rows: float32 [2, 16, 8192], P('section', ('groups', 'rank')), parts along dimension 1
The draws below stay inside these ranges and needn't reach their ends.
There are 2 independent parts, one for each index of `groups`. The reference program is written for one: setup_inputs(seed, part) draws one part's arguments, and reference() takes and returns one part's arrays. A program takes and returns all parts, laid end to end along the dimension named above; an argument that names none is the same for every part. Nothing has to cross between parts.
Inputs may be any that keep to these rules, and one draw needn't show every extreme that they name: Each section holds at least one request whose length is 256; lengths vary widely from request to request.
All inputs are finite; a program needn't handle non-finite values.
Results may differ from the reference program's by a relative error of at most 0.0022.
Values may be sent and summed in bfloat16 or wider, within the bound.
A program may use at most 128 MiB of HBM per device.

```python
import jax
import jax.numpy as jnp
from jax import lax

D = 8192
H = 64
KVH = 8
HD = 128
FF = 14336
CTX = 256
REQUESTS = 8
N_SECTION = 2


def drawn_draw(key, shape):
    return jax.random.truncated_normal(key, -6.0, 6.0, shape, jnp.float32)


def draw_rows_in(key, part):
    first, second, third = jax.random.split(jax.random.fold_in(key, 11), 3)
    row_scale = jnp.exp(jax.random.uniform(first, (N_SECTION, REQUESTS, 1), jnp.float32, jnp.log(0.3), jnp.log(3.0)))
    col_scale = jnp.exp(jax.random.uniform(second, (N_SECTION, 1, D), jnp.float32, jnp.log(0.3), jnp.log(3.0)))
    noise = jax.random.truncated_normal(third, -6.0, 6.0, (N_SECTION, REQUESTS, D), jnp.float32)
    return noise * row_scale * col_scale


def draw_query(key, part):
    base = drawn_draw(jax.random.fold_in(key, 1), (N_SECTION, REQUESTS, H * HD))
    return base.astype(jnp.bfloat16)


def draw_key_cache(key, part):
    base = drawn_draw(jax.random.fold_in(key, 2), (N_SECTION, REQUESTS, CTX, KVH * HD))
    return base.astype(jnp.bfloat16)


def draw_key_new(key, part):
    base = drawn_draw(jax.random.fold_in(key, 3), (N_SECTION, REQUESTS, KVH * HD))
    return base.astype(jnp.bfloat16)


def draw_lengths(key, part):
    first, second, third = jax.random.split(jax.random.fold_in(key, 21), 3)
    base = jax.random.randint(first, (N_SECTION, REQUESTS), 1, CTX + 1)
    shift_power = jax.random.randint(second, (N_SECTION, REQUESTS), 0, 4)
    shrunk = jnp.maximum(base // jnp.left_shift(jnp.ones_like(shift_power), shift_power), 1)
    longest = jax.random.randint(third, (N_SECTION, 1), 0, REQUESTS)
    places = jnp.arange(REQUESTS, dtype=jnp.int32)[None, :]
    return jnp.where(places == longest, CTX, shrunk).astype(jnp.int32)


def shard_levels(own_key, shape, cuts, smallest, top_value):
    factor_of, own = 1.0, jax.random.fold_in(own_key, 6)
    for dim, shards_of in cuts:
        steps = jnp.exp(jax.random.uniform(jax.random.fold_in(own, dim), (shards_of,), jnp.float32, smallest / len(cuts), top_value / len(cuts)))
        factor_of = factor_of * jnp.repeat(steps, shape[dim] // shards_of).reshape([-1 if axis == dim else 1 for axis in range(len(shape))])
    return factor_of


def bell_draw(own_key, dims, deviation, most, cuts=(), kind=jnp.bfloat16):
    array = jax.random.normal(own_key, dims, jnp.float32) * deviation
    if len(cuts) > 0:
        array = shard_levels(own_key, dims, cuts, -0.22, 0.18) * array
    return jnp.clip(array, min=-most, max=most).astype(kind)


def setup_inputs(seed: int = 0, part: int = 0) -> dict:
    splits = jax.random.split(jax.random.key(seed), 11)
    part_keys = jax.random.split(jax.random.fold_in(splits[10], part), 11)
    rows_in = draw_rows_in(jax.random.fold_in(jax.random.fold_in(splits[10], part), 71), part)
    query = draw_query(jax.random.fold_in(jax.random.fold_in(splits[10], part), 71), part)
    key_cache = draw_key_cache(jax.random.fold_in(jax.random.fold_in(splits[10], part), 71), part)
    value_cache = bell_draw(part_keys[3], (N_SECTION, REQUESTS, CTX, KVH * HD), 1.0, 6.0, ((0, 2), (1, 8)))
    key_new = draw_key_new(jax.random.fold_in(jax.random.fold_in(splits[10], part), 71), part)
    value_new = bell_draw(part_keys[5], (N_SECTION, REQUESTS, KVH * HD), 1.0, 6.0, ((0, 2), (1, 8)))
    lengths = draw_lengths(jax.random.fold_in(jax.random.fold_in(splits[10], part), 71), part)
    norm_gain = jnp.clip(1.0 + 0.15 * jax.random.normal(splits[7], (N_SECTION, D), jnp.float32), 0.25, 1.75)
    w_up = bell_draw(splits[8], (N_SECTION, D, FF), D ** -0.5, 0.0625, ((0, 2), (2, 8)))
    w_down = bell_draw(splits[9], (N_SECTION, FF, D), FF ** -0.5, 0.046875, ((0, 2), (1, 8)))
    return {"rows_in": rows_in, "query": query, "key_cache": key_cache, "value_cache": value_cache, "key_new": key_new, "value_new": value_new, "lengths": lengths, "norm_gain": norm_gain, "w_up": w_up, "w_down": w_down}


def attend(query, key_cache, value_cache, key_new, value_new, length):
    groups = H // KVH
    score_scale = HD ** (-0.5)
    queries = query.astype(jnp.float32).reshape(KVH, groups, HD)
    keys = key_cache.astype(jnp.float32).reshape(CTX, KVH, HD)
    scores = jnp.einsum('kgd,pkd->kgp', queries, keys) * score_scale
    live = jnp.arange(CTX, dtype=jnp.int32) < length
    scores = jnp.where(live[None, None, :], scores, jnp.float32(-1e+30))
    own = jnp.einsum('kgd,kd->kg', queries, key_new.astype(jnp.float32).reshape(KVH, HD)) * score_scale
    top = jnp.maximum(lax.optimization_barrier(jnp.max(scores, axis=-1)), own)
    powers = jnp.exp(scores - top[..., None])
    own_power = jnp.exp(own - top)
    total = lax.optimization_barrier(jnp.sum(powers, axis=-1)) + own_power
    probs = (powers / total[..., None]).astype(jnp.bfloat16)
    own_prob = (own_power / total).astype(jnp.bfloat16)
    values = value_cache.astype(jnp.float32).reshape(CTX, KVH, HD)
    result = jnp.einsum('kgp,pkd->kgd', probs.astype(jnp.float32), values)
    result = result + own_prob.astype(jnp.float32)[..., None] * value_new.astype(jnp.float32).reshape(KVH, 1, HD)
    return result.reshape(H * HD)

def reference(rows_in, query, key_cache, value_cache, key_new, value_new, lengths, norm_gain, w_up, w_down):
    attended = jax.vmap(jax.vmap(attend))(query, key_cache, value_cache, key_new, value_new, lengths)
    mixed = rows_in + attended
    scaled = mixed * lax.rsqrt(lax.optimization_barrier(jnp.mean(mixed * mixed, axis=-1, keepdims=True)) + 1e-05)
    normed = (scaled * norm_gain[:, None, :]).astype(jnp.bfloat16)
    outputs = []
    for section_index in range(N_SECTION):
        upward = jnp.dot(normed[section_index], w_up[section_index], preferred_element_type=jnp.float32)
        hidden = jax.nn.silu(upward).astype(jnp.bfloat16)
        down = jnp.dot(hidden, w_down[section_index], preferred_element_type=jnp.float32)
        outputs.append(mixed[section_index] + down)
    layer_out = jnp.stack(outputs, axis=0)
    return jnp.roll(layer_out, 1, axis=0)
```

```python
import functools

import jax
import jax.numpy as jnp
from jax import lax
from jax.experimental import pallas as pl
from jax.experimental.pallas import tpu as pltpu
from jax.sharding import PartitionSpec as P

HD = 128
EPS = 1e-05
LANE = 128
KV_CUTS = 2
ROW_CHUNKS = 2
UP_CHUNKS = 4
DOWN_CHUNKS = 4
PIECES = 2
MESH = pl.DeviceIdType.MESH


def attend(q, keys, values, key_new, value_new, length):
    heads, slots = q.shape[0], keys.shape[0]
    kvh = key_new.shape[0]
    per = heads // kvh
    scale = HD ** (-0.5)
    scores, owns = [], []
    for g in range(kvh):
        q_g = q[g * per : (g + 1) * per]
        scores.append(
            lax.dot_general(
                q_g.astype(jnp.bfloat16),
                keys[:, g * HD : (g + 1) * HD],
                (((1,), (1,)), ((), ())),
                preferred_element_type=jnp.float32,
            )
        )
        owns.append(jnp.sum(q_g * key_new[g : g + 1], axis=-1, keepdims=True))
    scores = jnp.concatenate(scores, axis=0) * scale
    own = jnp.concatenate(owns, axis=0) * scale
    live = lax.broadcasted_iota(jnp.int32, (heads, slots), 1) < length
    scores = jnp.where(live, scores, jnp.float32(-1e30))
    top = jnp.maximum(jnp.max(scores, axis=-1, keepdims=True), own)
    powers = jnp.exp(scores - top)
    own_power = jnp.exp(own - top)
    total = jnp.sum(powers, axis=-1, keepdims=True) + own_power
    probs = powers / total
    own_prob = (own_power / total).astype(jnp.bfloat16).astype(jnp.float32)
    out = []
    for g in range(kvh):
        rows = slice(g * per, (g + 1) * per)
        part = jnp.dot(
            probs[rows].astype(jnp.bfloat16),
            values[:, g * HD : (g + 1) * HD],
            preferred_element_type=jnp.float32,
        )
        out.append(part + own_prob[rows] * value_new[g : g + 1])
    return jnp.concatenate(out, axis=0)


def partner(me, step, count):
    other, bit = 0, 1
    while bit < count:
        digit = lax.rem(lax.div(me, bit), 2)
        other = other + bit * (1 - digit if step // bit % 2 else digit)
        bit *= 2
    return other


def far_first(n_groups, n_rank):
    steps = range(n_groups * n_rank)
    return sorted(steps, key=lambda s: (-(s % n_rank // 2), -(s // n_rank), -(s % 2)))


def heads_of(row):
    count = row.shape[1] // HD
    return jnp.concatenate([row[:, h * HD : (h + 1) * HD] for h in range(count)], axis=0)


def layer_kernel(
    sizes, pieces,
    len_in, rows_ref, q_ref, kc_ref, vc_ref, kn_ref, vn_ref, gain_ref, up_ref, down_ref,
    out_ref,
    rows_v, q_v, kc_v, vc_v, kn_v, vn_v, gain_v, up_v, down_v,
    mixed_v, mixed_in, mine, gathered, spread, acc, passing, passed, hidden, partial, sending,
    landed,
    len_ref, small_sem, kv_sem, up_sem, down_sem, mixed_sem, gsend, grecv, xsem, rsend, rrecv,
):
    n_groups, n_section, n_rank = sizes
    count = n_rank * n_groups
    group, section, rank = (lax.axis_index(a) for a in ("groups", "section", "rank"))
    me = group * n_rank + rank
    after = lax.rem(section + 1, n_section)
    order = far_first(n_groups, n_rank)
    up_chunks, depth = up_v.shape[0], up_v.shape[1]
    down_chunks, width = down_v.shape[0], down_v.shape[2]
    row_chunks, row_sub = gathered.shape[0], gathered.shape[2]
    part_sub = width // LANE
    half = up_chunks * depth
    base = pl.multiple_of(group * half, LANE)

    def place(peer, which):
        return {
            "groups": lax.div(peer, n_rank), "section": which, "rank": lax.rem(peer, n_rank)
        }

    small = [
        pltpu.make_async_copy(src, dst, small_sem.at[i])
        for i, (src, dst) in enumerate(
            (
                (q_ref, q_v), (kn_ref, kn_v), (len_in, len_ref),
                (vn_ref, vn_v), (rows_ref, rows_v), (gain_ref, gain_v),
            )
        )
    ]
    cut = kc_v.shape[0] // KV_CUTS
    caches = [
        pltpu.make_async_copy(
            ref.at[0, 0, pl.ds(i * cut, cut)], dst.at[pl.ds(i * cut, cut)], kv_sem.at[which, i]
        )
        for which, (ref, dst) in enumerate(((kc_ref, kc_v), (vc_ref, vc_v)))
        for i in range(KV_CUTS)
    ]
    for copy in small[:3] + caches[:KV_CUTS] + small[3:] + caches[KV_CUTS:]:
        copy.start()

    barrier = pltpu.get_barrier_semaphore()
    for shift in range(n_section):
        for step in range(count):
            if shift or step:
                pl.semaphore_signal(
                    barrier,
                    inc=1,
                    device_id=place(partner(me, step, count), lax.rem(section + shift, n_section)),
                    device_id_type=MESH,
                )

    ups = [
        pltpu.make_async_copy(
            up_ref.at[0, pl.ds(base + c * depth, depth)], up_v.at[c], up_sem.at[c]
        )
        for c in range(up_chunks)
    ]
    downs = [
        pltpu.make_async_copy(
            down_ref.at[0, :, pl.ds(base + c * width, width)], down_v.at[c], down_sem.at[c]
        )
        for c in range(down_chunks)
    ]
    for copy in ups + downs:
        copy.start()

    for copy in small + caches:
        copy.wait()
    attended = attend(
        heads_of(q_v[0].astype(jnp.float32)),
        kc_v[...],
        vc_v[...],
        heads_of(kn_v[0].astype(jnp.float32)),
        heads_of(vn_v[0].astype(jnp.float32)),
        len_ref[0, 0],
    )
    mixed = rows_v[...] + attended
    mixed_v[...] = mixed
    square = jnp.sum(jnp.sum(mixed * mixed, axis=-1, keepdims=True), axis=0, keepdims=True)
    scaled = mixed * lax.rsqrt(square / (mixed.shape[0] * mixed.shape[1]) + EPS)
    normed = (scaled * gain_v[...]).astype(jnp.bfloat16)
    for p in range(n_groups):
        for c in range(row_chunks):
            at = (p * row_chunks + c) * row_sub
            mine[p, c] = normed[at : at + row_sub]

    pl.semaphore_wait(barrier, n_section * count - 1)

    def row_copy(c, peer):
        return pltpu.make_async_remote_copy(
            src_ref=mine.at[lax.div(peer, n_rank), c],
            dst_ref=gathered.at[c, me],
            send_sem=gsend.at[c, peer],
            recv_sem=grecv.at[c, me],
            device_id=place(peer, section),
            device_id_type=MESH,
        )

    def row_landing(c, owner):
        return pltpu.make_async_remote_copy(
            src_ref=mine.at[0, c],
            dst_ref=gathered.at[c, owner],
            send_sem=gsend.at[c, owner],
            recv_sem=grecv.at[c, owner],
            device_id=place(owner, section),
            device_id_type=MESH,
        )

    @pl.loop(0, row_chunks)
    def _(c):
        for step in order:
            if step:
                row_copy(c, partner(me, step, count)).start()

    mixed_copy = pltpu.make_async_remote_copy(
        src_ref=mixed_v,
        dst_ref=mixed_in,
        send_sem=mixed_sem.at[0],
        recv_sem=mixed_sem.at[1],
        device_id=place(me, after),
        device_id_type=MESH,
    )
    mixed_copy.start()
    for c in range(row_chunks):
        gathered[c, me] = mine[group, c]

    def rows_of(c):
        for step in range(1, count):
            row_landing(c, partner(me, step, count)).wait_recv()
        for r in range(count):
            spread[r * row_sub : (r + 1) * row_sub] = gathered[c, r].astype(jnp.float32)
        return jnp.concatenate(
            [spread[pl.ds(j, count, stride=row_sub), :] for j in range(row_sub)], axis=1
        ).astype(jnp.bfloat16)

    def piece_copy(p):
        at, size = pieces[p]
        return pltpu.make_async_remote_copy(
            src_ref=passing.at[:, pl.ds(at, size)],
            dst_ref=passed.at[:, pl.ds(at, size)],
            send_sem=xsem.at[0, p],
            recv_sem=xsem.at[1, p],
            device_id={"groups": 1 - group, "section": section, "rank": rank},
            device_id_type=MESH,
        )

    per = up_chunks // row_chunks
    for c in range(row_chunks):
        block = rows_of(c)
        for k in range(per):
            ups[c * per + k].wait()
        weights = [up_v.at[c * per + k] for k in range(per)]
        blocks = [block[:, k * depth : (k + 1) * depth] for k in range(per)]
        last = c == row_chunks - 1
        for p, (at, size) in enumerate(pieces):
            total = acc[:, at : at + size] if c else 0.0
            for k in range(per):
                total = total + jnp.dot(
                    blocks[k], weights[k][:, at : at + size], preferred_element_type=jnp.float32
                )
            acc[:, at : at + size] = total
            if last:
                passing[:, at : at + size] = total.astype(jnp.bfloat16)
                piece_copy(p).start()

    for p, (at, size) in enumerate(pieces):
        piece_copy(p).wait_recv()
        upward = acc[:, at : at + size] + passed[:, at : at + size].astype(jnp.float32)
        hidden[:, at : at + size] = (upward / (1.0 + jnp.exp(-upward))).astype(jnp.bfloat16)

    def part_copy(c, peer):
        return pltpu.make_async_remote_copy(
            src_ref=sending.at[c, peer],
            dst_ref=landed.at[me, c],
            send_sem=rsend.at[c, peer],
            recv_sem=rrecv.at[c, me],
            device_id=place(peer, after),
            device_id_type=MESH,
        )

    def part_landing(c, owner):
        return pltpu.make_async_remote_copy(
            src_ref=sending.at[c, owner],
            dst_ref=landed.at[owner, c],
            send_sem=rsend.at[c, owner],
            recv_sem=rrecv.at[c, owner],
            device_id=place(owner, after),
            device_id_type=MESH,
        )

    @pl.loop(0, down_chunks)
    def _(c):
        pltpu.make_async_copy(
            down_ref.at[0, :, pl.ds(0, width)], down_v.at[c], down_sem.at[c]
        ).wait()
        lowered = jnp.dot(hidden[...], down_v[c], preferred_element_type=jnp.float32)
        for j in range(part_sub):
            partial[pl.ds(j, count, stride=part_sub), :] = lowered[:, j * LANE : (j + 1) * LANE]
        for r in range(count):
            sending[c, r] = partial[r * part_sub : (r + 1) * part_sub].astype(jnp.bfloat16)
        for step in order:
            part_copy(c, partner(me, step, count)).start()

    mixed_copy.wait_recv()

    @pl.loop(0, down_chunks)
    def _(c):
        for step in range(count):
            part_landing(c, partner(me, step, count)).wait_recv()
        for p in range(n_groups):
            rows = pl.ds(pl.multiple_of((p * down_chunks + c) * part_sub, part_sub), part_sub)
            total = mixed_in[rows]
            for r in range(n_rank):
                total = total + landed[p * n_rank + r, c].astype(jnp.float32)
            out_ref[rows] = total

    mixed_copy.wait_send()
    for p in range(len(pieces)):
        piece_copy(p).wait_send()

    @pl.loop(0, row_chunks)
    def _(c):
        for step in range(1, count):
            row_landing(c, partner(me, step, count)).wait_send()

    @pl.loop(0, down_chunks)
    def _(c):
        for step in range(count):
            part_landing(c, partner(me, step, count)).wait_send()


def fused(
    mesh_sizes, rows_in, query, key_cache, value_cache, key_new, value_new, lengths, norm_gain,
    w_up, w_down,
):
    n_groups, n_section, n_rank = mesh_sizes
    count = n_rank * n_groups
    d, slots, kv = rows_in.shape[-1], key_cache.shape[2], key_cache.shape[3]
    units = w_up.shape[2]
    heads, kvh, half = d // HD, kv // HD, d // n_groups
    depth, width = half // UP_CHUNKS, half // DOWN_CHUNKS
    row_sub, part_sub = half // ROW_CHUNKS // LANE, width // LANE
    first = -(-units // (256 * PIECES)) * 256
    pieces = [(at, min(first, units - at)) for at in range(0, units, first)]
    f32, bf16 = jnp.float32, jnp.bfloat16
    anywhere = pl.BlockSpec(memory_space=pltpu.HBM)
    out = pl.pallas_call(
        functools.partial(layer_kernel, mesh_sizes, pieces),
        out_shape=jax.ShapeDtypeStruct((heads, HD), f32),
        in_specs=[anywhere] * 10,
        out_specs=pl.BlockSpec(memory_space=pltpu.VMEM),
        scratch_shapes=[
            pltpu.VMEM((heads, HD), f32),
            pltpu.VMEM((1, 1, d), bf16),
            pltpu.VMEM((slots, kv), bf16),
            pltpu.VMEM((slots, kv), bf16),
            pltpu.VMEM((1, 1, kv), bf16),
            pltpu.VMEM((1, 1, kv), bf16),
            pltpu.VMEM((heads, HD), f32),
            pltpu.VMEM((UP_CHUNKS, depth, units), bf16),
            pltpu.VMEM((DOWN_CHUNKS, units, width), bf16),
            pltpu.VMEM((heads, HD), f32),
            pltpu.VMEM((heads, HD), f32),
            pltpu.VMEM((n_groups, ROW_CHUNKS, row_sub, LANE), bf16),
            pltpu.VMEM((ROW_CHUNKS, count, row_sub, LANE), bf16),
            pltpu.VMEM((count * row_sub, LANE), f32),
            pltpu.VMEM((count, units), f32),
            pltpu.VMEM((count, units), bf16),
            pltpu.VMEM((count, units), bf16),
            pltpu.VMEM((count, units), bf16),
            pltpu.VMEM((count * part_sub, LANE), f32),
            pltpu.VMEM((DOWN_CHUNKS, count, part_sub, LANE), bf16),
            pltpu.VMEM((count, DOWN_CHUNKS, part_sub, LANE), bf16),
            pltpu.SMEM((1, 1), jnp.int32),
            pltpu.SemaphoreType.DMA((6,)),
            pltpu.SemaphoreType.DMA((2, KV_CUTS)),
            pltpu.SemaphoreType.DMA((UP_CHUNKS,)),
            pltpu.SemaphoreType.DMA((DOWN_CHUNKS,)),
            pltpu.SemaphoreType.DMA((2,)),
            pltpu.SemaphoreType.DMA((ROW_CHUNKS, count)),
            pltpu.SemaphoreType.DMA((ROW_CHUNKS, count)),
            pltpu.SemaphoreType.DMA((2, len(pieces))),
            pltpu.SemaphoreType.DMA((DOWN_CHUNKS, count)),
            pltpu.SemaphoreType.DMA((DOWN_CHUNKS, count)),
        ],
        compiler_params=pltpu.CompilerParams(
            collective_id=0, has_side_effects=True, vmem_limit_bytes=64 * 1024 * 1024 - 65536
        ),
        name="layer",
    )(
        lengths,
        rows_in.reshape(heads, HD),
        query,
        key_cache,
        value_cache,
        key_new,
        value_new,
        norm_gain.reshape(heads, HD),
        w_up,
        w_down,
    )
    return out.reshape(1, 1, d)


def attend_plain(query, key_cache, value_cache, key_new, value_new, length):
    kv = key_cache.shape[1] // HD
    out = attend(
        query.reshape(-1, HD).astype(jnp.float32),
        key_cache,
        value_cache,
        key_new.reshape(kv, HD).astype(jnp.float32),
        value_new.reshape(kv, HD).astype(jnp.float32),
        length,
    )
    return out.reshape(-1)


def plain(
    rows_in, query, key_cache, value_cache, key_new, value_new, lengths, norm_gain, w_up, w_down
):
    section_rows = rows_in[0]
    local_rows = section_rows.shape[0]
    attended = jax.vmap(attend_plain)(
        query[0], key_cache[0], value_cache[0], key_new[0], value_new[0], lengths[0]
    )
    mixed = section_rows + attended
    scaled = mixed * lax.rsqrt(jnp.mean(mixed * mixed, axis=-1, keepdims=True) + EPS)
    normed = (scaled * norm_gain[0][None, :]).astype(jnp.bfloat16)
    upward = jnp.dot(
        lax.all_gather(normed, "rank", axis=0, tiled=True),
        w_up[0],
        preferred_element_type=jnp.float32,
    )
    hidden = jax.nn.silu(upward).astype(jnp.bfloat16)
    whole = lax.psum(jnp.dot(hidden, w_down[0], preferred_element_type=jnp.float32), "rank")
    mine = lax.dynamic_slice_in_dim(whole, lax.axis_index("rank") * local_rows, local_rows, 0)
    size = lax.axis_size("section")
    pairs = [(source, (source + 1) % size) for source in range(size)]
    return lax.ppermute(mixed + mine, "section", pairs)[None]


def solution(mesh):
    n_groups, n_section, n_rank = (mesh.shape[a] for a in ("groups", "section", "rank"))
    sizes = (n_groups, n_section, n_rank)
    count = n_groups * n_rank

    def per_device(*args):
        rows, d = args[0].shape[1], args[0].shape[2]
        slots, units = args[2].shape[2], args[8].shape[2]
        fits = (
            rows == 1
            and n_groups == 2
            and n_section > 1
            and count & (count - 1) == 0
            and count <= 32
            and units % LANE == 0
            and slots % (16 * KV_CUTS) == 0
            and d % (16 * LANE * n_groups * ROW_CHUNKS) == 0
            and d % (LANE * n_groups * UP_CHUNKS) == 0
            and d % (8 * LANE * n_groups * DOWN_CHUNKS) == 0
            and 4 * d // n_groups * units < 60 * 1000 * 1000
        )
        if fits:
            return fused(sizes, *args)
        return plain(*args)

    placed = (
        P("section", ("groups", "rank"), None),
        P("section", ("groups", "rank"), None),
        P("section", ("groups", "rank"), None, None),
        P("section", ("groups", "rank"), None, None),
        P("section", ("groups", "rank"), None),
        P("section", ("groups", "rank"), None),
        P("section", ("groups", "rank")),
        P("section", None),
        P("section", None, "rank"),
        P("section", "rank", None),
    )
    return jax.shard_map(
        per_device,
        mesh=mesh,
        in_specs=placed,
        out_specs=P("section", ("groups", "rank"), None),
        check_vma=False,
    )
```

```python
import functools

import jax
import jax.numpy as jnp
from jax import lax
from jax.experimental import pallas as pl
from jax.experimental.pallas import tpu as pltpu
from jax.sharding import PartitionSpec as P

HD = 128
EPS = 1e-05
LANE = 128
UP_CHUNKS = 4
PIECE = 512
WIDTH = 1024
MESH = pl.DeviceIdType.MESH


def attend(q, keys, values, key_new, value_new, length):
    heads, slots = q.shape[0], keys.shape[0]
    kvh = key_new.shape[0]
    per = heads // kvh
    scale = HD ** (-0.5)
    scores, owns = [], []
    for g in range(kvh):
        q_g = q[g * per : (g + 1) * per]
        scores.append(
            lax.dot_general(
                q_g.astype(jnp.bfloat16),
                keys[:, g * HD : (g + 1) * HD],
                (((1,), (1,)), ((), ())),
                preferred_element_type=jnp.float32,
            )
        )
        owns.append(jnp.sum(q_g * key_new[g : g + 1], axis=-1, keepdims=True))
    scores = jnp.concatenate(scores, axis=0) * scale
    own = jnp.concatenate(owns, axis=0) * scale
    live = lax.broadcasted_iota(jnp.int32, (heads, slots), 1) < length
    scores = jnp.where(live, scores, jnp.float32(-1e30))
    top = jnp.maximum(jnp.max(scores, axis=-1, keepdims=True), own)
    powers = jnp.exp(scores - top)
    own_power = jnp.exp(own - top)
    total = jnp.sum(powers, axis=-1, keepdims=True) + own_power
    probs = powers / total
    own_prob = (own_power / total).astype(jnp.bfloat16).astype(jnp.float32)
    out = []
    for g in range(kvh):
        rows = slice(g * per, (g + 1) * per)
        part = jnp.dot(
            probs[rows].astype(jnp.bfloat16),
            values[:, g * HD : (g + 1) * HD],
            preferred_element_type=jnp.float32,
        )
        out.append(part + own_prob[rows] * value_new[g : g + 1])
    return jnp.concatenate(out, axis=0)


def partner(me, step, count):
    other, bit = 0, 1
    while bit < count:
        digit = lax.rem(lax.div(me, bit), 2)
        other = other + bit * (1 - digit if step // bit % 2 else digit)
        bit *= 2
    return other


def far_first(n_groups, n_rank):
    steps = range(n_groups * n_rank)
    return sorted(steps, key=lambda s: (-(s % n_rank // 2), -(s // n_rank), -(s % 2)))


def heads_of(row):
    count = row.shape[1] // HD
    return jnp.concatenate([row[:, h * HD : (h + 1) * HD] for h in range(count)], axis=0)


def layer_kernel(
    sizes, pieces,
    len_in, rows_ref, q_ref, kc_ref, vc_ref, kn_ref, vn_ref, gain_ref, up_ref, down_ref,
    out_ref,
    rows_v, q_v, kc_v, vc_v, kn_v, vn_v, gain_v, up_v, down_v,
    mixed_v, mixed_in, mine, gathered, spread, acc, passing, passed, lowered, sending, landed,
    len_ref, small_sem, up_sem, down_sem, mixed_sem, gather_sem, piece_sem, part_sem,
):
    n_groups, n_section, n_rank = sizes
    count = n_rank * n_groups
    group, section, rank = (lax.axis_index(a) for a in ("groups", "section", "rank"))
    me = group * n_rank + rank
    after = lax.rem(section + 1, n_section)
    order = far_first(n_groups, n_rank)
    up_chunks, depth = up_v.shape[0], up_v.shape[1]
    half = up_chunks * depth
    sub = half // LANE
    base = pl.multiple_of(group * half, LANE)

    def place(peer, which):
        return {
            "groups": lax.div(peer, n_rank), "section": which, "rank": lax.rem(peer, n_rank)
        }

    small = [
        pltpu.make_async_copy(src, dst, small_sem.at[i])
        for i, (src, dst) in enumerate(
            (
                (q_ref, q_v), (kc_ref.at[0, 0], kc_v), (kn_ref, kn_v), (len_in, len_ref),
                (vc_ref.at[0, 0], vc_v), (vn_ref, vn_v), (rows_ref, rows_v), (gain_ref, gain_v),
            )
        )
    ]
    for copy in small:
        copy.start()

    barrier = pltpu.get_barrier_semaphore()
    for step in order:
        for shift in range(n_section):
            if shift or step:
                pl.semaphore_signal(
                    barrier,
                    inc=1,
                    device_id=place(partner(me, step, count), lax.rem(section + shift, n_section)),
                    device_id_type=MESH,
                )

    ups = [
        pltpu.make_async_copy(
            up_ref.at[0, pl.ds(base + c * depth, depth)], up_v.at[c], up_sem.at[c]
        )
        for c in range(up_chunks)
    ]
    downs = [
        pltpu.make_async_copy(
            down_ref.at[0, pl.ds(at, size), pl.ds(base, half)],
            down_v.at[pl.ds(at, size)],
            down_sem.at[p],
        )
        for p, (at, size) in enumerate(pieces)
    ]
    for copy in ups + downs:
        copy.start()

    for copy in small:
        copy.wait()
    attended = attend(
        heads_of(q_v[0].astype(jnp.float32)),
        kc_v[...],
        vc_v[...],
        heads_of(kn_v[0].astype(jnp.float32)),
        heads_of(vn_v[0].astype(jnp.float32)),
        len_ref[0, 0],
    )
    mixed = rows_v[...] + attended
    mixed_v[...] = mixed
    square = jnp.sum(jnp.sum(mixed * mixed, axis=-1, keepdims=True), axis=0, keepdims=True)
    scaled = mixed * lax.rsqrt(square / (mixed.shape[0] * mixed.shape[1]) + EPS)
    normed = (scaled * gain_v[...]).astype(jnp.bfloat16)
    for p in range(n_groups):
        mine[p] = normed[p * sub : (p + 1) * sub]

    pl.semaphore_wait(barrier, n_section * count - 1)

    for step in order:
        if step:
            peer = partner(me, step, count)
            pltpu.make_async_remote_copy(
                src_ref=mine.at[lax.div(peer, n_rank)],
                dst_ref=gathered.at[me],
                send_sem=gather_sem.at[0],
                recv_sem=gather_sem.at[1],
                device_id=place(peer, section),
                device_id_type=MESH,
            ).start()
    mixed_copy = pltpu.make_async_remote_copy(
        src_ref=mixed_v,
        dst_ref=mixed_in,
        send_sem=mixed_sem.at[0],
        recv_sem=mixed_sem.at[1],
        device_id=place(me, after),
        device_id_type=MESH,
    )
    mixed_copy.start()
    gathered[me] = mine[group]

    others = gathered.at[pl.ds(0, count - 1)]
    pltpu.make_async_copy(others, others, gather_sem.at[1]).wait()
    for r in range(count):
        spread[r * sub : (r + 1) * sub] = gathered[r].astype(jnp.float32)
    block = jnp.concatenate(
        [spread[pl.ds(j, count, stride=sub), :] for j in range(sub)], axis=1
    ).astype(jnp.bfloat16)

    def piece_copy(p):
        at, size = pieces[p]
        return pltpu.make_async_remote_copy(
            src_ref=passing.at[:, pl.ds(at, size)],
            dst_ref=passed.at[:, pl.ds(at, size)],
            send_sem=piece_sem.at[0, p],
            recv_sem=piece_sem.at[1, p],
            device_id={"groups": 1 - group, "section": section, "rank": rank},
            device_id_type=MESH,
        )

    for copy in ups:
        copy.wait()
    for p, (at, size) in enumerate(pieces):
        total = 0.0
        for k in range(up_chunks):
            total = total + jnp.dot(
                block[:, k * depth : (k + 1) * depth],
                up_v[k, :, at : at + size],
                preferred_element_type=jnp.float32,
            )
        acc[:, at : at + size] = total
        passing[:, at : at + size] = total.astype(jnp.bfloat16)
        piece_copy(p).start()

    for p, (at, size) in enumerate(pieces):
        downs[p].wait()
        piece_copy(p).wait_recv()
        upward = acc[:, at : at + size] + passed[:, at : at + size].astype(jnp.float32)
        hidden = (upward / (1.0 + jnp.exp(-upward))).astype(jnp.bfloat16)
        for n in range(0, half, WIDTH):
            cols = slice(n, n + WIDTH)
            part = jnp.dot(
                hidden, down_v[at : at + size, cols], preferred_element_type=jnp.float32
            )
            lowered[:, cols] = lowered[:, cols] + part if p else part

    for j in range(sub):
        spread[pl.ds(j, count, stride=sub), :] = lowered[:, j * LANE : (j + 1) * LANE]
    for r in range(count):
        sending[r] = spread[r * sub : (r + 1) * sub].astype(jnp.bfloat16)
    for step in order:
        peer = partner(me, step, count)
        pltpu.make_async_remote_copy(
            src_ref=sending.at[peer],
            dst_ref=landed.at[me],
            send_sem=part_sem.at[0],
            recv_sem=part_sem.at[1],
            device_id=place(peer, after),
            device_id_type=MESH,
        ).start()

    mixed_copy.wait_recv()
    pltpu.make_async_copy(landed, landed, part_sem.at[1]).wait()
    for p in range(n_groups):
        rows = slice(p * sub, (p + 1) * sub)
        total = mixed_in[rows]
        for r in range(n_rank):
            total = total + landed[p * n_rank + r].astype(jnp.float32)
        out_ref[rows] = total

    mixed_copy.wait_send()
    for p in range(len(pieces)):
        piece_copy(p).wait_send()
    pltpu.make_async_copy(others, others, gather_sem.at[0]).wait()
    pltpu.make_async_copy(sending, sending, part_sem.at[0]).wait()


def fused(
    mesh_sizes, rows_in, query, key_cache, value_cache, key_new, value_new, lengths, norm_gain,
    w_up, w_down,
):
    n_groups, n_section, n_rank = mesh_sizes
    count = n_rank * n_groups
    d, slots, kv = rows_in.shape[-1], key_cache.shape[2], key_cache.shape[3]
    units = w_up.shape[2]
    heads, kvh, half = d // HD, kv // HD, d // n_groups
    depth, sub = half // UP_CHUNKS, half // LANE
    pieces = [(at, min(PIECE, units - at)) for at in range(0, units, PIECE)]
    f32, bf16 = jnp.float32, jnp.bfloat16
    anywhere = pl.BlockSpec(memory_space=pltpu.HBM)
    out = pl.pallas_call(
        functools.partial(layer_kernel, mesh_sizes, pieces),
        out_shape=jax.ShapeDtypeStruct((heads, HD), f32),
        in_specs=[anywhere] * 10,
        out_specs=pl.BlockSpec(memory_space=pltpu.VMEM),
        scratch_shapes=[
            pltpu.VMEM((heads, HD), f32),
            pltpu.VMEM((1, 1, d), bf16),
            pltpu.VMEM((slots, kv), bf16),
            pltpu.VMEM((slots, kv), bf16),
            pltpu.VMEM((1, 1, kv), bf16),
            pltpu.VMEM((1, 1, kv), bf16),
            pltpu.VMEM((heads, HD), f32),
            pltpu.VMEM((UP_CHUNKS, depth, units), bf16),
            pltpu.VMEM((units, half), bf16),
            pltpu.VMEM((heads, HD), f32),
            pltpu.VMEM((heads, HD), f32),
            pltpu.VMEM((n_groups, sub, LANE), bf16),
            pltpu.VMEM((count, sub, LANE), bf16),
            pltpu.VMEM((count * sub, LANE), f32),
            pltpu.VMEM((count, units), f32),
            pltpu.VMEM((count, units), bf16),
            pltpu.VMEM((count, units), bf16),
            pltpu.VMEM((count, half), f32),
            pltpu.VMEM((count, sub, LANE), bf16),
            pltpu.VMEM((count, sub, LANE), bf16),
            pltpu.SMEM((1, 1), jnp.int32),
            pltpu.SemaphoreType.DMA((8,)),
            pltpu.SemaphoreType.DMA((UP_CHUNKS,)),
            pltpu.SemaphoreType.DMA((len(pieces),)),
            pltpu.SemaphoreType.DMA((2,)),
            pltpu.SemaphoreType.DMA((2,)),
            pltpu.SemaphoreType.DMA((2, len(pieces))),
            pltpu.SemaphoreType.DMA((2,)),
        ],
        compiler_params=pltpu.CompilerParams(
            collective_id=0, has_side_effects=True, vmem_limit_bytes=64 * 1024 * 1024 - 65536
        ),
        name="layer",
    )(
        lengths,
        rows_in.reshape(heads, HD),
        query,
        key_cache,
        value_cache,
        key_new,
        value_new,
        norm_gain.reshape(heads, HD),
        w_up,
        w_down,
    )
    return out.reshape(1, 1, d)


def attend_plain(query, key_cache, value_cache, key_new, value_new, length):
    kv = key_cache.shape[1] // HD
    out = attend(
        query.reshape(-1, HD).astype(jnp.float32),
        key_cache,
        value_cache,
        key_new.reshape(kv, HD).astype(jnp.float32),
        value_new.reshape(kv, HD).astype(jnp.float32),
        length,
    )
    return out.reshape(-1)


def plain(
    rows_in, query, key_cache, value_cache, key_new, value_new, lengths, norm_gain, w_up, w_down
):
    section_rows = rows_in[0]
    local_rows = section_rows.shape[0]
    attended = jax.vmap(attend_plain)(
        query[0], key_cache[0], value_cache[0], key_new[0], value_new[0], lengths[0]
    )
    mixed = section_rows + attended
    scaled = mixed * lax.rsqrt(jnp.mean(mixed * mixed, axis=-1, keepdims=True) + EPS)
    normed = (scaled * norm_gain[0][None, :]).astype(jnp.bfloat16)
    upward = jnp.dot(
        lax.all_gather(normed, "rank", axis=0, tiled=True),
        w_up[0],
        preferred_element_type=jnp.float32,
    )
    hidden = jax.nn.silu(upward).astype(jnp.bfloat16)
    whole = lax.psum(jnp.dot(hidden, w_down[0], preferred_element_type=jnp.float32), "rank")
    mine = lax.dynamic_slice_in_dim(whole, lax.axis_index("rank") * local_rows, local_rows, 0)
    size = lax.axis_size("section")
    pairs = [(source, (source + 1) % size) for source in range(size)]
    return lax.ppermute(mixed + mine, "section", pairs)[None]


def solution(mesh):
    n_groups, n_section, n_rank = (mesh.shape[a] for a in ("groups", "section", "rank"))
    sizes = (n_groups, n_section, n_rank)
    count = n_groups * n_rank

    def per_device(*args):
        rows, d = args[0].shape[1], args[0].shape[2]
        units = args[8].shape[2]
        fits = (
            rows == 1
            and n_groups == 2
            and n_section > 1
            and count & (count - 1) == 0
            and count <= 32
            and units % LANE == 0
            and d % (16 * LANE * n_groups) == 0
            and d % (WIDTH * n_groups) == 0
            and d % (LANE * n_groups * UP_CHUNKS) == 0
            and 4 * d // n_groups * units < 60 * 1000 * 1000
        )
        if fits:
            return fused(sizes, *args)
        return plain(*args)

    placed = (
        P("section", ("groups", "rank"), None),
        P("section", ("groups", "rank"), None),
        P("section", ("groups", "rank"), None, None),
        P("section", ("groups", "rank"), None, None),
        P("section", ("groups", "rank"), None),
        P("section", ("groups", "rank"), None),
        P("section", ("groups", "rank")),
        P("section", None),
        P("section", None, "rank"),
        P("section", "rank", None),
    )
    return jax.shard_map(
        per_device,
        mesh=mesh,
        in_specs=placed,
        out_specs=P("section", ("groups", "rank"), None),
        check_vma=False,
    )
```

```python
import functools

import jax
import jax.numpy as jnp
from jax import lax
from jax.experimental import pallas as pl
from jax.experimental.pallas import tpu as pltpu
from jax.sharding import PartitionSpec as P

HD = 128
EPS = 1e-05
LANE = 128
UP_CHUNKS = 4
PIECE = 512
WIDTH = 1024
LEAD = 2
SPLIT = 3
MESH = pl.DeviceIdType.MESH


def attend(q, keys, values, key_new, value_new, length):
    heads, slots = q.shape[0], keys.shape[0]
    kvh = key_new.shape[0]
    per = heads // kvh
    scale = HD ** (-0.5)
    scores, owns = [], []
    for g in range(kvh):
        q_g = q[g * per : (g + 1) * per]
        scores.append(
            lax.dot_general(
                q_g.astype(jnp.bfloat16),
                keys[:, g * HD : (g + 1) * HD],
                (((1,), (1,)), ((), ())),
                preferred_element_type=jnp.float32,
            )
        )
        owns.append(jnp.sum(q_g * key_new[g : g + 1], axis=-1, keepdims=True))
    scores = jnp.concatenate(scores, axis=0) * scale
    own = jnp.concatenate(owns, axis=0) * scale
    live = lax.broadcasted_iota(jnp.int32, (heads, slots), 1) < length
    scores = jnp.where(live, scores, jnp.float32(-1e30))
    top = jnp.maximum(jnp.max(scores, axis=-1, keepdims=True), own)
    powers = jnp.exp(scores - top)
    own_power = jnp.exp(own - top)
    total = jnp.sum(powers, axis=-1, keepdims=True) + own_power
    probs = powers / total
    own_prob = (own_power / total).astype(jnp.bfloat16).astype(jnp.float32)
    out = []
    for g in range(kvh):
        rows = slice(g * per, (g + 1) * per)
        part = jnp.dot(
            probs[rows].astype(jnp.bfloat16),
            values[:, g * HD : (g + 1) * HD],
            preferred_element_type=jnp.float32,
        )
        out.append(part + own_prob[rows] * value_new[g : g + 1])
    return jnp.concatenate(out, axis=0)


def partner(me, step, count):
    other, bit = 0, 1
    while bit < count:
        digit = lax.rem(lax.div(me, bit), 2)
        other = other + bit * (1 - digit if step // bit % 2 else digit)
        bit *= 2
    return other


def far_first(n_groups, n_rank):
    steps = range(n_groups * n_rank)
    return sorted(steps, key=lambda s: (-(s % n_rank // 2), -(s // n_rank), -(s % 2)))


def heads_of(row):
    count = row.shape[1] // HD
    return jnp.concatenate([row[:, h * HD : (h + 1) * HD] for h in range(count)], axis=0)


def layer_kernel(
    sizes, pieces,
    len_in, rows_ref, q_ref, kc_ref, vc_ref, kn_ref, vn_ref, gain_ref, up_ref, down_ref,
    out_ref,
    rows_v, q_v, kc_v, vc_v, kn_v, vn_v, gain_v, up_v, down_v,
    mixed_v, mixed_in, mine, gathered, spread, acc, passing, passed, lowered, sending, landed,
    len_ref, small_sem, up_sem, down_sem, mixed_sem, gather_sem, piece_sem, part_sem, turn,
):
    n_groups, n_section, n_rank = sizes
    count = n_rank * n_groups
    group, section, rank = (lax.axis_index(a) for a in ("groups", "section", "rank"))
    me = group * n_rank + rank
    after = lax.rem(section + 1, n_section)
    order = far_first(n_groups, n_rank)
    root_first = sorted(range(count), key=lambda p: p % n_rank // 2 + p % 2 + p // n_rank)
    up_chunks, depth = up_v.shape[0], up_v.shape[1]
    half = up_chunks * depth
    sub = half // LANE
    base = pl.multiple_of(group * half, LANE)

    def place(peer, which):
        return {
            "groups": lax.div(peer, n_rank), "section": which, "rank": lax.rem(peer, n_rank)
        }

    small = [
        pltpu.make_async_copy(src, dst, small_sem.at[i])
        for i, (src, dst) in enumerate(
            (
                (q_ref, q_v), (kc_ref.at[0, 0], kc_v), (kn_ref, kn_v), (len_in, len_ref),
                (vc_ref.at[0, 0], vc_v), (vn_ref, vn_v), (rows_ref, rows_v), (gain_ref, gain_v),
            )
        )
    ]
    for copy in small:
        copy.start()

    ups = [
        pltpu.make_async_copy(
            up_ref.at[0, pl.ds(base + c * depth, depth)], up_v.at[c], up_sem.at[c]
        )
        for c in range(up_chunks)
    ]
    downs = [
        pltpu.make_async_copy(
            down_ref.at[0, pl.ds(at, size), pl.ds(base, half)],
            down_v.at[pl.ds(at, size)],
            down_sem.at[p],
        )
        for p, (at, size) in enumerate(pieces)
    ]

    barrier = pltpu.get_barrier_semaphore()
    for step in order:
        for shift in range(n_section):
            if shift or step:
                pl.semaphore_signal(
                    barrier,
                    inc=1,
                    device_id=place(partner(me, step, count), lax.rem(section + shift, n_section)),
                    device_id_type=MESH,
                )

    for copy in ups:
        copy.start()
    for copy in small:
        copy.wait()
    attended = attend(
        heads_of(q_v[0].astype(jnp.float32)),
        kc_v[...],
        vc_v[...],
        heads_of(kn_v[0].astype(jnp.float32)),
        heads_of(vn_v[0].astype(jnp.float32)),
        len_ref[0, 0],
    )
    mixed = rows_v[...] + attended
    mixed_v[...] = mixed
    square = jnp.sum(jnp.sum(mixed * mixed, axis=-1, keepdims=True), axis=0, keepdims=True)
    scaled = mixed * lax.rsqrt(square / (mixed.shape[0] * mixed.shape[1]) + EPS)
    normed = (scaled * gain_v[...]).astype(jnp.bfloat16)
    for p in range(n_groups):
        mine[p] = normed[p * sub : (p + 1) * sub]

    pl.semaphore_wait(barrier, n_section * count - 1)

    def row_copy(peer, sem):
        return pltpu.make_async_remote_copy(
            src_ref=mine.at[lax.div(peer, n_rank)],
            dst_ref=gathered.at[me],
            send_sem=gather_sem.at[sem],
            recv_sem=gather_sem.at[1],
            device_id=place(peer, section),
            device_id_type=MESH,
        )

    far = [step for step in order if step % n_rank >= n_rank // 2]
    near = [step for step in order if step and step not in far]
    lead = gathered.at[pl.ds(0, LEAD)]

    @pl.when(section == 0)
    def _():
        for step in far[:LEAD]:
            row_copy(partner(me, step, count), 0).start()
        for step in far[LEAD:] + near:
            row_copy(partner(me, step, count), 2).start()
        pltpu.make_async_copy(lead, lead, gather_sem.at[0]).wait()
        pl.semaphore_signal(turn, inc=1, device_id={"section": after}, device_id_type=MESH)

    @pl.when(section != 0)
    def _():
        for step in far[:SPLIT] + near:
            row_copy(partner(me, step, count), 2).start()
        pl.semaphore_wait(turn, 1)
        for step in far[SPLIT:]:
            row_copy(partner(me, step, count), 2).start()

    mixed_copy = pltpu.make_async_remote_copy(
        src_ref=mixed_v,
        dst_ref=mixed_in,
        send_sem=mixed_sem.at[0],
        recv_sem=mixed_sem.at[1],
        device_id=place(me, after),
        device_id_type=MESH,
    )
    mixed_copy.start()
    gathered[me] = mine[group]
    for copy in downs:
        copy.start()

    others = gathered.at[pl.ds(0, count - 1)]
    pltpu.make_async_copy(others, others, gather_sem.at[1]).wait()
    for r in range(count):
        spread[r * sub : (r + 1) * sub] = gathered[r].astype(jnp.float32)
    block = jnp.concatenate(
        [spread[pl.ds(j, count, stride=sub), :] for j in range(sub)], axis=1
    ).astype(jnp.bfloat16)

    def piece_copy(p):
        at, size = pieces[p]
        return pltpu.make_async_remote_copy(
            src_ref=passing.at[:, pl.ds(at, size)],
            dst_ref=passed.at[:, pl.ds(at, size)],
            send_sem=piece_sem.at[0, p],
            recv_sem=piece_sem.at[1, p],
            device_id={"groups": 1 - group, "section": section, "rank": rank},
            device_id_type=MESH,
        )

    for copy in ups:
        copy.wait()
    for p, (at, size) in enumerate(pieces):
        total = 0.0
        for k in range(up_chunks):
            total = total + jnp.dot(
                block[:, k * depth : (k + 1) * depth],
                up_v[k, :, at : at + size],
                preferred_element_type=jnp.float32,
            )
        acc[:, at : at + size] = total
        passing[:, at : at + size] = total.astype(jnp.bfloat16)
        piece_copy(p).start()

    for p, (at, size) in enumerate(pieces):
        downs[p].wait()
        piece_copy(p).wait_recv()
        upward = acc[:, at : at + size] + passed[:, at : at + size].astype(jnp.float32)
        hidden = (upward / (1.0 + jnp.exp(-upward))).astype(jnp.bfloat16)
        for n in range(0, half, WIDTH):
            cols = slice(n, n + WIDTH)
            part = jnp.dot(
                hidden, down_v[at : at + size, cols], preferred_element_type=jnp.float32
            )
            lowered[:, cols] = lowered[:, cols] + part if p else part

    for j in range(sub):
        spread[pl.ds(j, count, stride=sub), :] = lowered[:, j * LANE : (j + 1) * LANE]
    for r in range(count):
        sending[r] = spread[r * sub : (r + 1) * sub].astype(jnp.bfloat16)
    for peer in root_first:
        pltpu.make_async_remote_copy(
            src_ref=sending.at[peer],
            dst_ref=landed.at[me],
            send_sem=part_sem.at[0],
            recv_sem=part_sem.at[1],
            device_id=place(peer, after),
            device_id_type=MESH,
        ).start()

    mixed_copy.wait_recv()
    pltpu.make_async_copy(landed, landed, part_sem.at[1]).wait()
    for p in range(n_groups):
        rows = slice(p * sub, (p + 1) * sub)
        total = mixed_in[rows]
        for r in range(n_rank):
            total = total + landed[p * n_rank + r].astype(jnp.float32)
        out_ref[rows] = total

    mixed_copy.wait_send()
    for p in range(len(pieces)):
        piece_copy(p).wait_send()
    @pl.when(section == 0)
    def _():
        rest = gathered.at[pl.ds(0, count - 1 - LEAD)]
        pltpu.make_async_copy(rest, rest, gather_sem.at[2]).wait()

    @pl.when(section != 0)
    def _():
        pltpu.make_async_copy(others, others, gather_sem.at[2]).wait()

    pltpu.make_async_copy(sending, sending, part_sem.at[0]).wait()


def fused(
    mesh_sizes, rows_in, query, key_cache, value_cache, key_new, value_new, lengths, norm_gain,
    w_up, w_down,
):
    n_groups, n_section, n_rank = mesh_sizes
    count = n_rank * n_groups
    d, slots, kv = rows_in.shape[-1], key_cache.shape[2], key_cache.shape[3]
    units = w_up.shape[2]
    heads, kvh, half = d // HD, kv // HD, d // n_groups
    depth, sub = half // UP_CHUNKS, half // LANE
    pieces = [(at, min(PIECE, units - at)) for at in range(0, units, PIECE)]
    f32, bf16 = jnp.float32, jnp.bfloat16
    anywhere = pl.BlockSpec(memory_space=pltpu.HBM)
    out = pl.pallas_call(
        functools.partial(layer_kernel, mesh_sizes, pieces),
        out_shape=jax.ShapeDtypeStruct((heads, HD), f32),
        in_specs=[anywhere] * 10,
        out_specs=pl.BlockSpec(memory_space=pltpu.VMEM),
        scratch_shapes=[
            pltpu.VMEM((heads, HD), f32),
            pltpu.VMEM((1, 1, d), bf16),
            pltpu.VMEM((slots, kv), bf16),
            pltpu.VMEM((slots, kv), bf16),
            pltpu.VMEM((1, 1, kv), bf16),
            pltpu.VMEM((1, 1, kv), bf16),
            pltpu.VMEM((heads, HD), f32),
            pltpu.VMEM((UP_CHUNKS, depth, units), bf16),
            pltpu.VMEM((units, half), bf16),
            pltpu.VMEM((heads, HD), f32),
            pltpu.VMEM((heads, HD), f32),
            pltpu.VMEM((n_groups, sub, LANE), bf16),
            pltpu.VMEM((count, sub, LANE), bf16),
            pltpu.VMEM((count * sub, LANE), f32),
            pltpu.VMEM((count, units), f32),
            pltpu.VMEM((count, units), bf16),
            pltpu.VMEM((count, units), bf16),
            pltpu.VMEM((count, half), f32),
            pltpu.VMEM((count, sub, LANE), bf16),
            pltpu.VMEM((count, sub, LANE), bf16),
            pltpu.SMEM((1, 1), jnp.int32),
            pltpu.SemaphoreType.DMA((8,)),
            pltpu.SemaphoreType.DMA((UP_CHUNKS,)),
            pltpu.SemaphoreType.DMA((len(pieces),)),
            pltpu.SemaphoreType.DMA((2,)),
            pltpu.SemaphoreType.DMA((3,)),
            pltpu.SemaphoreType.DMA((2, len(pieces))),
            pltpu.SemaphoreType.DMA((2,)),
            pltpu.SemaphoreType.REGULAR,
        ],
        compiler_params=pltpu.CompilerParams(
            collective_id=0, has_side_effects=True, vmem_limit_bytes=64 * 1024 * 1024 - 65536
        ),
        name="layer",
    )(
        lengths,
        rows_in.reshape(heads, HD),
        query,
        key_cache,
        value_cache,
        key_new,
        value_new,
        norm_gain.reshape(heads, HD),
        w_up,
        w_down,
    )
    return out.reshape(1, 1, d)


def attend_plain(query, key_cache, value_cache, key_new, value_new, length):
    kv = key_cache.shape[1] // HD
    out = attend(
        query.reshape(-1, HD).astype(jnp.float32),
        key_cache,
        value_cache,
        key_new.reshape(kv, HD).astype(jnp.float32),
        value_new.reshape(kv, HD).astype(jnp.float32),
        length,
    )
    return out.reshape(-1)


def plain(
    rows_in, query, key_cache, value_cache, key_new, value_new, lengths, norm_gain, w_up, w_down
):
    section_rows = rows_in[0]
    local_rows = section_rows.shape[0]
    attended = jax.vmap(attend_plain)(
        query[0], key_cache[0], value_cache[0], key_new[0], value_new[0], lengths[0]
    )
    mixed = section_rows + attended
    scaled = mixed * lax.rsqrt(jnp.mean(mixed * mixed, axis=-1, keepdims=True) + EPS)
    normed = (scaled * norm_gain[0][None, :]).astype(jnp.bfloat16)
    upward = jnp.dot(
        lax.all_gather(normed, "rank", axis=0, tiled=True),
        w_up[0],
        preferred_element_type=jnp.float32,
    )
    hidden = jax.nn.silu(upward).astype(jnp.bfloat16)
    whole = lax.psum(jnp.dot(hidden, w_down[0], preferred_element_type=jnp.float32), "rank")
    mine = lax.dynamic_slice_in_dim(whole, lax.axis_index("rank") * local_rows, local_rows, 0)
    size = lax.axis_size("section")
    pairs = [(source, (source + 1) % size) for source in range(size)]
    return lax.ppermute(mixed + mine, "section", pairs)[None]


def solution(mesh):
    n_groups, n_section, n_rank = (mesh.shape[a] for a in ("groups", "section", "rank"))
    sizes = (n_groups, n_section, n_rank)
    count = n_groups * n_rank

    def per_device(*args):
        rows, d = args[0].shape[1], args[0].shape[2]
        units = args[8].shape[2]
        fits = (
            rows == 1
            and n_groups == 2
            and n_section == 2
            and n_rank >= 8
            and count & (count - 1) == 0
            and count <= 32
            and units % LANE == 0
            and d % (16 * LANE * n_groups) == 0
            and d % (WIDTH * n_groups) == 0
            and d % (LANE * n_groups * UP_CHUNKS) == 0
            and 4 * d // n_groups * units < 60 * 1000 * 1000
        )
        if fits:
            return fused(sizes, *args)
        return plain(*args)

    placed = (
        P("section", ("groups", "rank"), None),
        P("section", ("groups", "rank"), None),
        P("section", ("groups", "rank"), None, None),
        P("section", ("groups", "rank"), None, None),
        P("section", ("groups", "rank"), None),
        P("section", ("groups", "rank"), None),
        P("section", ("groups", "rank")),
        P("section", None),
        P("section", None, "rank"),
        P("section", "rank", None),
    )
    return jax.shard_map(
        per_device,
        mesh=mesh,
        in_specs=placed,
        out_specs=P("section", ("groups", "rank"), None),
        check_vma=False,
    )
```

```python
import functools

import jax
import jax.numpy as jnp
from jax import lax
from jax.experimental import pallas as pl
from jax.experimental.pallas import tpu as pltpu
from jax.sharding import PartitionSpec as P

HD = 128
EPS = 1e-05
LANE = 128
UP_CHUNKS = 4
PIECE = 1024
WIDTH = 1024
LEAD = 2
SPLIT = 3
MESH = pl.DeviceIdType.MESH


def attend(q, keys, values, key_new, value_new, length):
    heads, slots = q.shape[0], keys.shape[0]
    kvh = key_new.shape[0]
    per = heads // kvh
    scale = HD ** (-0.5)
    scores, owns = [], []
    for g in range(kvh):
        q_g = q[g * per : (g + 1) * per]
        scores.append(
            lax.dot_general(
                q_g.astype(jnp.bfloat16),
                keys[:, g * HD : (g + 1) * HD],
                (((1,), (1,)), ((), ())),
                preferred_element_type=jnp.float32,
            )
        )
        owns.append(jnp.sum(q_g * key_new[g : g + 1], axis=-1, keepdims=True))
    scores = jnp.concatenate(scores, axis=0) * scale
    own = jnp.concatenate(owns, axis=0) * scale
    live = lax.broadcasted_iota(jnp.int32, (heads, slots), 1) < length
    scores = jnp.where(live, scores, jnp.float32(-1e30))
    top = jnp.maximum(jnp.max(scores, axis=-1, keepdims=True), own)
    powers = jnp.exp(scores - top)
    own_power = jnp.exp(own - top)
    total = jnp.sum(powers, axis=-1, keepdims=True) + own_power
    probs = powers / total
    own_prob = (own_power / total).astype(jnp.bfloat16).astype(jnp.float32)
    out = []
    for g in range(kvh):
        rows = slice(g * per, (g + 1) * per)
        part = jnp.dot(
            probs[rows].astype(jnp.bfloat16),
            values[:, g * HD : (g + 1) * HD],
            preferred_element_type=jnp.float32,
        )
        out.append(part + own_prob[rows] * value_new[g : g + 1])
    return jnp.concatenate(out, axis=0)


def partner(me, step, count):
    other, bit = 0, 1
    while bit < count:
        digit = lax.rem(lax.div(me, bit), 2)
        other = other + bit * (1 - digit if step // bit % 2 else digit)
        bit *= 2
    return other


def far_first(n_groups, n_rank):
    steps = range(n_groups * n_rank)
    return sorted(steps, key=lambda s: (-(s % n_rank // 2), -(s // n_rank), -(s % 2)))


def heads_of(row):
    count = row.shape[1] // HD
    return jnp.concatenate([row[:, h * HD : (h + 1) * HD] for h in range(count)], axis=0)


def layer_kernel(
    sizes, pieces,
    len_in, rows_ref, q_ref, kc_ref, vc_ref, kn_ref, vn_ref, gain_ref, up_ref, down_ref,
    out_ref,
    rows_v, q_v, kc_v, vc_v, kn_v, vn_v, gain_v, up_v, down_v,
    mixed_v, mixed_in, mine, gathered, spread, acc, passing, passed, lowered, sending, landed,
    len_ref, small_sem, up_sem, down_sem, mixed_sem, gather_sem, piece_sem, part_sem, turn,
):
    n_groups, n_section, n_rank = sizes
    count = n_rank * n_groups
    group, section, rank = (lax.axis_index(a) for a in ("groups", "section", "rank"))
    me = group * n_rank + rank
    after = lax.rem(section + 1, n_section)
    order = far_first(n_groups, n_rank)
    root_first = sorted(range(count), key=lambda p: p % n_rank // 2 + p % 2 + p // n_rank)
    up_chunks, depth = up_v.shape[0], up_v.shape[1]
    half = up_chunks * depth
    sub = half // LANE
    base = pl.multiple_of(group * half, LANE)

    def place(peer, which):
        return {
            "groups": lax.div(peer, n_rank), "section": which, "rank": lax.rem(peer, n_rank)
        }

    small = [
        pltpu.make_async_copy(src, dst, small_sem.at[i])
        for i, (src, dst) in enumerate(
            (
                (q_ref, q_v), (kc_ref.at[0, 0], kc_v), (kn_ref, kn_v), (len_in, len_ref),
                (vc_ref.at[0, 0], vc_v), (vn_ref, vn_v), (rows_ref, rows_v), (gain_ref, gain_v),
            )
        )
    ]
    for copy in small:
        copy.start()

    ups = [
        pltpu.make_async_copy(
            up_ref.at[0, pl.ds(base + c * depth, depth)], up_v.at[c], up_sem.at[c]
        )
        for c in range(up_chunks)
    ]
    downs = [
        pltpu.make_async_copy(
            down_ref.at[0, pl.ds(at, size), pl.ds(base, half)],
            down_v.at[pl.ds(at, size)],
            down_sem.at[p],
        )
        for p, (at, size) in enumerate(pieces)
    ]

    barrier = pltpu.get_barrier_semaphore()
    for step in order:
        for shift in range(n_section):
            if shift or step:
                pl.semaphore_signal(
                    barrier,
                    inc=1,
                    device_id=place(partner(me, step, count), lax.rem(section + shift, n_section)),
                    device_id_type=MESH,
                )

    for copy in ups:
        copy.start()
    for copy in small:
        copy.wait()
    attended = attend(
        heads_of(q_v[0].astype(jnp.float32)),
        kc_v[...],
        vc_v[...],
        heads_of(kn_v[0].astype(jnp.float32)),
        heads_of(vn_v[0].astype(jnp.float32)),
        len_ref[0, 0],
    )
    mixed = rows_v[...] + attended
    mixed_v[...] = mixed
    square = jnp.sum(jnp.sum(mixed * mixed, axis=-1, keepdims=True), axis=0, keepdims=True)
    scaled = mixed * lax.rsqrt(square / (mixed.shape[0] * mixed.shape[1]) + EPS)
    normed = (scaled * gain_v[...]).astype(jnp.bfloat16)
    for p in range(n_groups):
        mine[p] = normed[p * sub : (p + 1) * sub]

    gathered[me] = mine[group]
    pl.semaphore_wait(barrier, n_section * count - 1)

    def row_copy(peer, sem):
        return pltpu.make_async_remote_copy(
            src_ref=mine.at[lax.div(peer, n_rank)],
            dst_ref=gathered.at[me],
            send_sem=gather_sem.at[sem],
            recv_sem=gather_sem.at[1],
            device_id=place(peer, section),
            device_id_type=MESH,
        )

    far = [step for step in order if step % n_rank >= n_rank // 2]
    near = [step for step in order if step and step not in far]
    lead = gathered.at[pl.ds(0, LEAD)]

    @pl.when(section == 0)
    def _():
        for step in far[:LEAD]:
            row_copy(partner(me, step, count), 0).start()
        for step in far[LEAD:] + near:
            row_copy(partner(me, step, count), 2).start()
        pltpu.make_async_copy(lead, lead, gather_sem.at[0]).wait()
        pl.semaphore_signal(turn, inc=1, device_id={"section": after}, device_id_type=MESH)

    @pl.when(section != 0)
    def _():
        for step in far[:SPLIT] + near:
            row_copy(partner(me, step, count), 2).start()
        pl.semaphore_wait(turn, 1)
        for step in far[SPLIT:]:
            row_copy(partner(me, step, count), 2).start()

    mixed_copy = pltpu.make_async_remote_copy(
        src_ref=mixed_v,
        dst_ref=mixed_in,
        send_sem=mixed_sem.at[0],
        recv_sem=mixed_sem.at[1],
        device_id=place(me, after),
        device_id_type=MESH,
    )
    mixed_copy.start()
    for copy in downs:
        copy.start()

    others = gathered.at[pl.ds(0, count - 1)]
    for copy in ups:
        copy.wait()
    pltpu.make_async_copy(others, others, gather_sem.at[1]).wait()
    for r in range(count):
        spread[r * sub : (r + 1) * sub] = gathered[r].astype(jnp.float32)
    block = jnp.concatenate(
        [spread[pl.ds(j, count, stride=sub), :] for j in range(sub)], axis=1
    ).astype(jnp.bfloat16)

    def piece_copy(p):
        at, size = pieces[p]
        return pltpu.make_async_remote_copy(
            src_ref=passing.at[:, pl.ds(at, size)],
            dst_ref=passed.at[:, pl.ds(at, size)],
            send_sem=piece_sem.at[len(pieces)],
            recv_sem=piece_sem.at[p],
            device_id={"groups": 1 - group, "section": section, "rank": rank},
            device_id_type=MESH,
        )

    for p, (at, size) in enumerate(pieces):
        total = 0.0
        for k in range(up_chunks):
            total = total + jnp.dot(
                block[:, k * depth : (k + 1) * depth],
                up_v[k, :, at : at + size],
                preferred_element_type=jnp.float32,
            )
        acc[:, at : at + size] = total
        passing[:, at : at + size] = total.astype(jnp.bfloat16)
        piece_copy(p).start()

    for p, (at, size) in enumerate(pieces):
        downs[p].wait()
        piece_copy(p).wait_recv()
        upward = acc[:, at : at + size] + passed[:, at : at + size].astype(jnp.float32)
        hidden = (upward / (1.0 + jnp.exp(-upward))).astype(jnp.bfloat16)
        for n in range(0, half, WIDTH):
            cols = slice(n, n + WIDTH)
            part = jnp.dot(
                hidden, down_v[at : at + size, cols], preferred_element_type=jnp.float32
            )
            total = lowered[:, cols] + part if p else part
            if p < len(pieces) - 1:
                lowered[:, cols] = total
            else:
                for j in range(WIDTH // LANE):
                    h = n // LANE + j
                    spread[h * count : (h + 1) * count] = total[:, j * LANE : (j + 1) * LANE]

    def part_copy(peer):
        return pltpu.make_async_remote_copy(
            src_ref=sending.at[peer],
            dst_ref=landed.at[me],
            send_sem=part_sem.at[0],
            recv_sem=part_sem.at[1],
            device_id=place(peer, after),
            device_id_type=MESH,
        )

    for i, peer in enumerate(root_first):
        sending[peer] = spread[pl.ds(peer, sub, stride=count), :].astype(jnp.bfloat16)
        if i:
            part_copy(root_first[i - 1]).start()
    part_copy(root_first[-1]).start()

    mixed_copy.wait_recv()
    pltpu.make_async_copy(landed, landed, part_sem.at[1]).wait()
    for p in range(n_groups):
        rows = slice(p * sub, (p + 1) * sub)
        total = mixed_in[rows]
        for r in range(n_rank):
            total = total + landed[p * n_rank + r].astype(jnp.float32)
        out_ref[rows] = total

    mixed_copy.wait_send()
    pltpu.make_async_copy(passing, passing, piece_sem.at[len(pieces)]).wait()
    @pl.when(section == 0)
    def _():
        rest = gathered.at[pl.ds(0, count - 1 - LEAD)]
        pltpu.make_async_copy(rest, rest, gather_sem.at[2]).wait()

    @pl.when(section != 0)
    def _():
        pltpu.make_async_copy(others, others, gather_sem.at[2]).wait()

    pltpu.make_async_copy(sending, sending, part_sem.at[0]).wait()


def fused(
    mesh_sizes, rows_in, query, key_cache, value_cache, key_new, value_new, lengths, norm_gain,
    w_up, w_down,
):
    n_groups, n_section, n_rank = mesh_sizes
    count = n_rank * n_groups
    d, slots, kv = rows_in.shape[-1], key_cache.shape[2], key_cache.shape[3]
    units = w_up.shape[2]
    heads, kvh, half = d // HD, kv // HD, d // n_groups
    depth, sub = half // UP_CHUNKS, half // LANE
    pieces = [(at, min(PIECE, units - at)) for at in range(0, units, PIECE)]
    f32, bf16 = jnp.float32, jnp.bfloat16
    anywhere = pl.BlockSpec(memory_space=pltpu.HBM)
    out = pl.pallas_call(
        functools.partial(layer_kernel, mesh_sizes, pieces),
        out_shape=jax.ShapeDtypeStruct((heads, HD), f32),
        in_specs=[anywhere] * 10,
        out_specs=pl.BlockSpec(memory_space=pltpu.VMEM),
        scratch_shapes=[
            pltpu.VMEM((heads, HD), f32),
            pltpu.VMEM((1, 1, d), bf16),
            pltpu.VMEM((slots, kv), bf16),
            pltpu.VMEM((slots, kv), bf16),
            pltpu.VMEM((1, 1, kv), bf16),
            pltpu.VMEM((1, 1, kv), bf16),
            pltpu.VMEM((heads, HD), f32),
            pltpu.VMEM((UP_CHUNKS, depth, units), bf16),
            pltpu.VMEM((units, half), bf16),
            pltpu.VMEM((heads, HD), f32),
            pltpu.VMEM((heads, HD), f32),
            pltpu.VMEM((n_groups, sub, LANE), bf16),
            pltpu.VMEM((count, sub, LANE), bf16),
            pltpu.VMEM((count * sub, LANE), f32),
            pltpu.VMEM((count, units), f32),
            pltpu.VMEM((count, units), bf16),
            pltpu.VMEM((count, units), bf16),
            pltpu.VMEM((count, half), f32),
            pltpu.VMEM((count, sub, LANE), bf16),
            pltpu.VMEM((count, sub, LANE), bf16),
            pltpu.SMEM((1, 1), jnp.int32),
            pltpu.SemaphoreType.DMA((8,)),
            pltpu.SemaphoreType.DMA((UP_CHUNKS,)),
            pltpu.SemaphoreType.DMA((len(pieces),)),
            pltpu.SemaphoreType.DMA((2,)),
            pltpu.SemaphoreType.DMA((3,)),
            pltpu.SemaphoreType.DMA((len(pieces) + 1,)),
            pltpu.SemaphoreType.DMA((2,)),
            pltpu.SemaphoreType.REGULAR,
        ],
        compiler_params=pltpu.CompilerParams(
            collective_id=0, has_side_effects=True, vmem_limit_bytes=64 * 1024 * 1024 - 65536
        ),
        name="layer",
    )(
        lengths,
        rows_in.reshape(heads, HD),
        query,
        key_cache,
        value_cache,
        key_new,
        value_new,
        norm_gain.reshape(heads, HD),
        w_up,
        w_down,
    )
    return out.reshape(1, 1, d)


def attend_plain(query, key_cache, value_cache, key_new, value_new, length):
    kv = key_cache.shape[1] // HD
    out = attend(
        query.reshape(-1, HD).astype(jnp.float32),
        key_cache,
        value_cache,
        key_new.reshape(kv, HD).astype(jnp.float32),
        value_new.reshape(kv, HD).astype(jnp.float32),
        length,
    )
    return out.reshape(-1)


def plain(
    rows_in, query, key_cache, value_cache, key_new, value_new, lengths, norm_gain, w_up, w_down
):
    section_rows = rows_in[0]
    local_rows = section_rows.shape[0]
    attended = jax.vmap(attend_plain)(
        query[0], key_cache[0], value_cache[0], key_new[0], value_new[0], lengths[0]
    )
    mixed = section_rows + attended
    scaled = mixed * lax.rsqrt(jnp.mean(mixed * mixed, axis=-1, keepdims=True) + EPS)
    normed = (scaled * norm_gain[0][None, :]).astype(jnp.bfloat16)
    upward = jnp.dot(
        lax.all_gather(normed, "rank", axis=0, tiled=True),
        w_up[0],
        preferred_element_type=jnp.float32,
    )
    hidden = jax.nn.silu(upward).astype(jnp.bfloat16)
    whole = lax.psum(jnp.dot(hidden, w_down[0], preferred_element_type=jnp.float32), "rank")
    mine = lax.dynamic_slice_in_dim(whole, lax.axis_index("rank") * local_rows, local_rows, 0)
    size = lax.axis_size("section")
    pairs = [(source, (source + 1) % size) for source in range(size)]
    return lax.ppermute(mixed + mine, "section", pairs)[None]


def solution(mesh):
    n_groups, n_section, n_rank = (mesh.shape[a] for a in ("groups", "section", "rank"))
    sizes = (n_groups, n_section, n_rank)
    count = n_groups * n_rank

    def per_device(*args):
        rows, d = args[0].shape[1], args[0].shape[2]
        units = args[8].shape[2]
        fits = (
            rows == 1
            and n_groups == 2
            and n_section == 2
            and n_rank >= 8
            and count & (count - 1) == 0
            and count <= 32
            and units % LANE == 0
            and d % (16 * LANE * n_groups) == 0
            and d % (WIDTH * n_groups) == 0
            and d % (LANE * n_groups * UP_CHUNKS) == 0
            and 4 * d // n_groups * units < 60 * 1000 * 1000
        )
        if fits:
            return fused(sizes, *args)
        return plain(*args)

    placed = (
        P("section", ("groups", "rank"), None),
        P("section", ("groups", "rank"), None),
        P("section", ("groups", "rank"), None, None),
        P("section", ("groups", "rank"), None, None),
        P("section", ("groups", "rank"), None),
        P("section", ("groups", "rank"), None),
        P("section", ("groups", "rank")),
        P("section", None),
        P("section", None, "rank"),
        P("section", "rank", None),
    )
    return jax.shard_map(
        per_device,
        mesh=mesh,
        in_specs=placed,
        out_specs=P("section", ("groups", "rank"), None),
        check_vma=False,
    )
```

```python
import functools

import jax
import jax.numpy as jnp
from jax import lax
from jax.experimental import pallas as pl
from jax.experimental.pallas import tpu as pltpu
from jax.sharding import PartitionSpec as P

HD = 128
EPS = 1e-05
LANE = 128
UP_CHUNKS = 4
PIECE = 1024
WIDTH = 1024
LEAD = 3
SPLIT = 3
MESH = pl.DeviceIdType.MESH


def attend(q, keys, values, key_new, value_new, length):
    heads, slots = q.shape[0], keys.shape[0]
    kvh = key_new.shape[0]
    per = heads // kvh
    scale = HD ** (-0.5)
    scores, owns = [], []
    for g in range(kvh):
        q_g = q[g * per : (g + 1) * per]
        scores.append(
            lax.dot_general(
                q_g.astype(jnp.bfloat16),
                keys[:, g * HD : (g + 1) * HD],
                (((1,), (1,)), ((), ())),
                preferred_element_type=jnp.float32,
            )
        )
        owns.append(jnp.sum(q_g * key_new[g : g + 1], axis=-1, keepdims=True))
    scores = jnp.concatenate(scores, axis=0) * scale
    own = jnp.concatenate(owns, axis=0) * scale
    live = lax.broadcasted_iota(jnp.int32, (heads, slots), 1) < length
    scores = jnp.where(live, scores, jnp.float32(-1e30))
    top = jnp.maximum(jnp.max(scores, axis=-1, keepdims=True), own)
    powers = jnp.exp(scores - top)
    own_power = jnp.exp(own - top)
    total = jnp.sum(powers, axis=-1, keepdims=True) + own_power
    probs = powers / total
    own_prob = (own_power / total).astype(jnp.bfloat16).astype(jnp.float32)
    out = []
    for g in range(kvh):
        rows = slice(g * per, (g + 1) * per)
        part = jnp.dot(
            probs[rows].astype(jnp.bfloat16),
            values[:, g * HD : (g + 1) * HD],
            preferred_element_type=jnp.float32,
        )
        out.append(part + own_prob[rows] * value_new[g : g + 1])
    return jnp.concatenate(out, axis=0)


def partner(me, step, count):
    other, bit = 0, 1
    while bit < count:
        digit = lax.rem(lax.div(me, bit), 2)
        other = other + bit * (1 - digit if step // bit % 2 else digit)
        bit *= 2
    return other


def far_first(n_groups, n_rank):
    steps = range(n_groups * n_rank)
    return sorted(steps, key=lambda s: (-(s % n_rank // 2), -(s // n_rank), -(s % 2)))


def heads_of(row):
    count = row.shape[1] // HD
    return jnp.concatenate([row[:, h * HD : (h + 1) * HD] for h in range(count)], axis=0)


def layer_kernel(
    sizes, pieces,
    len_in, rows_ref, q_ref, kc_ref, vc_ref, kn_ref, vn_ref, gain_ref, up_ref, down_ref,
    out_ref,
    rows_v, q_v, kc_v, vc_v, kn_v, vn_v, gain_v, up_v, down_v,
    mixed_v, mixed_in, mine, gathered, spread, acc, passing, passed, lowered, sending, landed,
    len_ref, small_sem, up_sem, down_sem, mixed_sem, gather_sem, piece_sem, part_sem, turn,
):
    n_groups, n_section, n_rank = sizes
    count = n_rank * n_groups
    group, section, rank = (lax.axis_index(a) for a in ("groups", "section", "rank"))
    me = group * n_rank + rank
    after = lax.rem(section + 1, n_section)
    order = far_first(n_groups, n_rank)
    root_first = sorted(range(count), key=lambda p: p % n_rank // 2 + p % 2 + p // n_rank)
    up_chunks, depth = up_v.shape[0], up_v.shape[1]
    half = up_chunks * depth
    sub = half // LANE
    base = pl.multiple_of(group * half, LANE)

    def place(peer, which):
        return {
            "groups": lax.div(peer, n_rank), "section": which, "rank": lax.rem(peer, n_rank)
        }

    small = [
        pltpu.make_async_copy(src, dst, small_sem.at[i])
        for i, (src, dst) in enumerate(
            (
                (q_ref, q_v), (kc_ref.at[0, 0], kc_v), (kn_ref, kn_v), (len_in, len_ref),
                (vc_ref.at[0, 0], vc_v), (vn_ref, vn_v), (rows_ref, rows_v), (gain_ref, gain_v),
            )
        )
    ]
    for copy in small:
        copy.start()

    ups = [
        pltpu.make_async_copy(
            up_ref.at[0, pl.ds(base + c * depth, depth)], up_v.at[c], up_sem.at[c]
        )
        for c in range(up_chunks)
    ]
    downs = [
        pltpu.make_async_copy(
            down_ref.at[0, pl.ds(at, size), pl.ds(base, half)],
            down_v.at[pl.ds(at, size)],
            down_sem.at[p],
        )
        for p, (at, size) in enumerate(pieces)
    ]

    barrier = pltpu.get_barrier_semaphore()
    for step in order:
        for shift in range(n_section):
            if shift or step:
                pl.semaphore_signal(
                    barrier,
                    inc=1,
                    device_id=place(partner(me, step, count), lax.rem(section + shift, n_section)),
                    device_id_type=MESH,
                )

    for copy in ups:
        copy.start()
    for copy in small:
        copy.wait()
    attended = attend(
        heads_of(q_v[0].astype(jnp.float32)),
        kc_v[...],
        vc_v[...],
        heads_of(kn_v[0].astype(jnp.float32)),
        heads_of(vn_v[0].astype(jnp.float32)),
        len_ref[0, 0],
    )
    mixed = rows_v[...] + attended
    mixed_v[...] = mixed
    square = jnp.sum(jnp.sum(mixed * mixed, axis=-1, keepdims=True), axis=0, keepdims=True)
    scaled = mixed * lax.rsqrt(square / (mixed.shape[0] * mixed.shape[1]) + EPS)
    normed = (scaled * gain_v[...]).astype(jnp.bfloat16)
    for p in range(n_groups):
        mine[p] = normed[p * sub : (p + 1) * sub]

    gathered[me] = mine[group]
    pl.semaphore_wait(barrier, n_section * count - 1)

    def row_copy(peer, sem):
        return pltpu.make_async_remote_copy(
            src_ref=mine.at[lax.div(peer, n_rank)],
            dst_ref=gathered.at[me],
            send_sem=gather_sem.at[sem],
            recv_sem=gather_sem.at[1],
            device_id=place(peer, section),
            device_id_type=MESH,
        )

    half_rank = n_rank // 2
    high = lax.div(rank, half_rank)
    far = []
    for z in range(half_rank // 2):
        for step in (3, 2, 1, 0):
            end = 2 * (half_rank - 1 - z) * (1 - high) + 2 * z * high
            side = lax.rem(rank, 2) if step % 2 == 0 else 1 - lax.rem(rank, 2)
            team = group if step < 2 else 1 - group
            far.append(team * n_rank + end + side)
    near = [
        partner(me, step, count) for step in order if step and step % n_rank < half_rank
    ]
    lead = gathered.at[pl.ds(0, LEAD)]

    @pl.when(section == 0)
    def _():
        for peer in far[:LEAD]:
            row_copy(peer, 0).start()
        for peer in far[LEAD:] + near:
            row_copy(peer, 2).start()
        pltpu.make_async_copy(lead, lead, gather_sem.at[0]).wait()
        pl.semaphore_signal(turn, inc=1, device_id={"section": after}, device_id_type=MESH)

    @pl.when(section != 0)
    def _():
        for peer in far[:SPLIT] + near:
            row_copy(peer, 2).start()
        pl.semaphore_wait(turn, 1)
        for peer in far[SPLIT:]:
            row_copy(peer, 2).start()

    mixed_copy = pltpu.make_async_remote_copy(
        src_ref=mixed_v,
        dst_ref=mixed_in,
        send_sem=mixed_sem.at[0],
        recv_sem=mixed_sem.at[1],
        device_id=place(me, after),
        device_id_type=MESH,
    )
    mixed_copy.start()
    for copy in downs:
        copy.start()

    others = gathered.at[pl.ds(0, count - 1)]
    for copy in ups:
        copy.wait()
    pltpu.make_async_copy(others, others, gather_sem.at[1]).wait()
    for r in range(count):
        spread[r * sub : (r + 1) * sub] = gathered[r].astype(jnp.float32)
    block = jnp.concatenate(
        [spread[pl.ds(j, count, stride=sub), :] for j in range(sub)], axis=1
    ).astype(jnp.bfloat16)

    def piece_copy(p):
        at, size = pieces[p]
        return pltpu.make_async_remote_copy(
            src_ref=passing.at[:, pl.ds(at, size)],
            dst_ref=passed.at[:, pl.ds(at, size)],
            send_sem=piece_sem.at[len(pieces)],
            recv_sem=piece_sem.at[p],
            device_id={"groups": 1 - group, "section": section, "rank": rank},
            device_id_type=MESH,
        )

    for p, (at, size) in enumerate(pieces):
        total = 0.0
        for k in range(up_chunks):
            total = total + jnp.dot(
                block[:, k * depth : (k + 1) * depth],
                up_v[k, :, at : at + size],
                preferred_element_type=jnp.float32,
            )
        acc[:, at : at + size] = total
        passing[:, at : at + size] = total.astype(jnp.bfloat16)
        piece_copy(p).start()

    for p, (at, size) in enumerate(pieces):
        downs[p].wait()
        piece_copy(p).wait_recv()
        upward = acc[:, at : at + size] + passed[:, at : at + size].astype(jnp.float32)
        hidden = (upward / (1.0 + jnp.exp(-upward))).astype(jnp.bfloat16)
        for n in range(0, half, WIDTH):
            cols = slice(n, n + WIDTH)
            part = jnp.dot(
                hidden, down_v[at : at + size, cols], preferred_element_type=jnp.float32
            )
            total = lowered[:, cols] + part if p else part
            if p < len(pieces) - 1:
                lowered[:, cols] = total
            else:
                for j in range(WIDTH // LANE):
                    h = n // LANE + j
                    spread[h * count : (h + 1) * count] = total[:, j * LANE : (j + 1) * LANE]

    def part_copy(peer):
        return pltpu.make_async_remote_copy(
            src_ref=sending.at[peer],
            dst_ref=landed.at[me],
            send_sem=part_sem.at[0],
            recv_sem=part_sem.at[1],
            device_id=place(peer, after),
            device_id_type=MESH,
        )

    for i, peer in enumerate(root_first):
        sending[peer] = spread[pl.ds(peer, sub, stride=count), :].astype(jnp.bfloat16)
        if i:
            part_copy(root_first[i - 1]).start()
    part_copy(root_first[-1]).start()

    mixed_copy.wait_recv()
    pltpu.make_async_copy(landed, landed, part_sem.at[1]).wait()
    for p in range(n_groups):
        rows = slice(p * sub, (p + 1) * sub)
        total = mixed_in[rows]
        for r in range(n_rank):
            total = total + landed[p * n_rank + r].astype(jnp.float32)
        out_ref[rows] = total

    mixed_copy.wait_send()
    pltpu.make_async_copy(passing, passing, piece_sem.at[len(pieces)]).wait()
    @pl.when(section == 0)
    def _():
        rest = gathered.at[pl.ds(0, count - 1 - LEAD)]
        pltpu.make_async_copy(rest, rest, gather_sem.at[2]).wait()

    @pl.when(section != 0)
    def _():
        pltpu.make_async_copy(others, others, gather_sem.at[2]).wait()

    pltpu.make_async_copy(sending, sending, part_sem.at[0]).wait()


def fused(
    mesh_sizes, rows_in, query, key_cache, value_cache, key_new, value_new, lengths, norm_gain,
    w_up, w_down,
):
    n_groups, n_section, n_rank = mesh_sizes
    count = n_rank * n_groups
    d, slots, kv = rows_in.shape[-1], key_cache.shape[2], key_cache.shape[3]
    units = w_up.shape[2]
    heads, kvh, half = d // HD, kv // HD, d // n_groups
    depth, sub = half // UP_CHUNKS, half // LANE
    pieces = [(at, min(PIECE, units - at)) for at in range(0, units, PIECE)]
    f32, bf16 = jnp.float32, jnp.bfloat16
    anywhere = pl.BlockSpec(memory_space=pltpu.HBM)
    out = pl.pallas_call(
        functools.partial(layer_kernel, mesh_sizes, pieces),
        out_shape=jax.ShapeDtypeStruct((heads, HD), f32),
        in_specs=[anywhere] * 10,
        out_specs=pl.BlockSpec(memory_space=pltpu.VMEM),
        scratch_shapes=[
            pltpu.VMEM((heads, HD), f32),
            pltpu.VMEM((1, 1, d), bf16),
            pltpu.VMEM((slots, kv), bf16),
            pltpu.VMEM((slots, kv), bf16),
            pltpu.VMEM((1, 1, kv), bf16),
            pltpu.VMEM((1, 1, kv), bf16),
            pltpu.VMEM((heads, HD), f32),
            pltpu.VMEM((UP_CHUNKS, depth, units), bf16),
            pltpu.VMEM((units, half), bf16),
            pltpu.VMEM((heads, HD), f32),
            pltpu.VMEM((heads, HD), f32),
            pltpu.VMEM((n_groups, sub, LANE), bf16),
            pltpu.VMEM((count, sub, LANE), bf16),
            pltpu.VMEM((count * sub, LANE), f32),
            pltpu.VMEM((count, units), f32),
            pltpu.VMEM((count, units), bf16),
            pltpu.VMEM((count, units), bf16),
            pltpu.VMEM((count, half), f32),
            pltpu.VMEM((count, sub, LANE), bf16),
            pltpu.VMEM((count, sub, LANE), bf16),
            pltpu.SMEM((1, 1), jnp.int32),
            pltpu.SemaphoreType.DMA((8,)),
            pltpu.SemaphoreType.DMA((UP_CHUNKS,)),
            pltpu.SemaphoreType.DMA((len(pieces),)),
            pltpu.SemaphoreType.DMA((2,)),
            pltpu.SemaphoreType.DMA((3,)),
            pltpu.SemaphoreType.DMA((len(pieces) + 1,)),
            pltpu.SemaphoreType.DMA((2,)),
            pltpu.SemaphoreType.REGULAR,
        ],
        compiler_params=pltpu.CompilerParams(
            collective_id=0, has_side_effects=True, vmem_limit_bytes=64 * 1024 * 1024 - 65536
        ),
        name="layer",
    )(
        lengths,
        rows_in.reshape(heads, HD),
        query,
        key_cache,
        value_cache,
        key_new,
        value_new,
        norm_gain.reshape(heads, HD),
        w_up,
        w_down,
    )
    return out.reshape(1, 1, d)


def attend_plain(query, key_cache, value_cache, key_new, value_new, length):
    kv = key_cache.shape[1] // HD
    out = attend(
        query.reshape(-1, HD).astype(jnp.float32),
        key_cache,
        value_cache,
        key_new.reshape(kv, HD).astype(jnp.float32),
        value_new.reshape(kv, HD).astype(jnp.float32),
        length,
    )
    return out.reshape(-1)


def plain(
    rows_in, query, key_cache, value_cache, key_new, value_new, lengths, norm_gain, w_up, w_down
):
    section_rows = rows_in[0]
    local_rows = section_rows.shape[0]
    attended = jax.vmap(attend_plain)(
        query[0], key_cache[0], value_cache[0], key_new[0], value_new[0], lengths[0]
    )
    mixed = section_rows + attended
    scaled = mixed * lax.rsqrt(jnp.mean(mixed * mixed, axis=-1, keepdims=True) + EPS)
    normed = (scaled * norm_gain[0][None, :]).astype(jnp.bfloat16)
    upward = jnp.dot(
        lax.all_gather(normed, "rank", axis=0, tiled=True),
        w_up[0],
        preferred_element_type=jnp.float32,
    )
    hidden = jax.nn.silu(upward).astype(jnp.bfloat16)
    whole = lax.psum(jnp.dot(hidden, w_down[0], preferred_element_type=jnp.float32), "rank")
    mine = lax.dynamic_slice_in_dim(whole, lax.axis_index("rank") * local_rows, local_rows, 0)
    size = lax.axis_size("section")
    pairs = [(source, (source + 1) % size) for source in range(size)]
    return lax.ppermute(mixed + mine, "section", pairs)[None]


def solution(mesh):
    n_groups, n_section, n_rank = (mesh.shape[a] for a in ("groups", "section", "rank"))
    sizes = (n_groups, n_section, n_rank)
    count = n_groups * n_rank

    def per_device(*args):
        rows, d = args[0].shape[1], args[0].shape[2]
        units = args[8].shape[2]
        fits = (
            rows == 1
            and n_groups == 2
            and n_section == 2
            and n_rank >= 8
            and count & (count - 1) == 0
            and count <= 32
            and units % LANE == 0
            and d % (16 * LANE * n_groups) == 0
            and d % (WIDTH * n_groups) == 0
            and d % (LANE * n_groups * UP_CHUNKS) == 0
            and 4 * d // n_groups * units < 60 * 1000 * 1000
        )
        if fits:
            return fused(sizes, *args)
        return plain(*args)

    placed = (
        P("section", ("groups", "rank"), None),
        P("section", ("groups", "rank"), None),
        P("section", ("groups", "rank"), None, None),
        P("section", ("groups", "rank"), None, None),
        P("section", ("groups", "rank"), None),
        P("section", ("groups", "rank"), None),
        P("section", ("groups", "rank")),
        P("section", None),
        P("section", None, "rank"),
        P("section", "rank", None),
    )
    return jax.shard_map(
        per_device,
        mesh=mesh,
        in_specs=placed,
        out_specs=P("section", ("groups", "rank"), None),
        check_vma=False,
    )
```
